32 devices in a mesh: row: 4 (over y, core), col: 8 (over z, x).
Axes of the slice: x: 2, y: 2, z: 4, core: 2. Of those that a mesh axis runs over, the one named last changes fastest.
Arguments:
- matrix: float32 [16384, 16384], P('row', 'col'), may hold values from -500 to 500
Outputs:
- reduced: float32 [16384, 16384], P('row', 'col')
The draws below stay inside these ranges and needn't reach their ends.
All inputs are finite; a program needn't handle non-finite values.
Results may differ from the reference program's by a relative error of at most 0.0003.
Values sent between devices are 32-bit elements; how exact they have to be, the bound alone decides.
No kernel may reach another device: no remote copies, remote signals or barrier semaphores. Data moves between devices by JAX's collectives and lax.ppermute only.
A program may use at most 192 MiB of HBM per device.

```python
import math
import jax
import jax.numpy as jnp
from jax import lax

N = 16384
REFL = 4
PANELS = 2


def draw_matrix(key, part):
    scale_key = jax.random.fold_in(key, 11)
    noise_key = jax.random.fold_in(key, 12)
    diagonal_key = jax.random.fold_in(key, 14)
    position_ramp = jnp.arange(N, dtype=jnp.float32) / N
    spread = jnp.exp(jax.random.uniform(scale_key, (N,), jnp.float32, math.log(0.33), math.log(3.3)))
    scales = spread * jnp.exp(0.5 * math.log(3.0) * position_ramp)
    entries = jax.random.truncated_normal(noise_key, -6.0, 6.0, (N, N), jnp.float32)
    symmetric = (entries + entries.T) * 0.7071
    stiffness = jax.random.uniform(diagonal_key, (N,), jnp.float32, 2.0, 6.0)
    return scales[:, None] * symmetric * scales[None, :] + jnp.diag(stiffness * scales * scales)


def setup_inputs(seed: int = 0) -> dict:
    arg_keys = jax.random.split(jax.random.key(seed), 2)
    matrix = draw_matrix(jax.random.fold_in(arg_keys[1], 71), 0)
    return dict(matrix=matrix)


highest = lax.Precision.HIGHEST

def product(left, right):
    return jnp.dot(left, right, precision=highest, preferred_element_type=jnp.float32)

def reference(matrix):
    total = matrix.shape[0]
    positions = jnp.arange(total, dtype=jnp.int32)
    current = matrix
    for panel_index in range(PANELS):
        reflectors = jnp.zeros((total, REFL), jnp.float32)
        updates = jnp.zeros((total, REFL), jnp.float32)
        for inner_index in range(REFL):
            target = panel_index * REFL + inner_index
            column = current[:, target] - product(reflectors, updates[target]) - product(updates, reflectors[target])
            beneath = jnp.where(positions > target, column, 0.0)
            length = jnp.sqrt(jnp.sum(beneath * beneath))
            leading = column[target + 1]
            signed = jnp.where(leading >= 0.0, length, -length)
            vector = beneath + jnp.where(positions == target + 1, signed, 0.0)
            factor = 1.0 / (length * (length + jnp.abs(leading)))
            against_updates = product(vector, updates)
            against_reflectors = product(vector, reflectors)
            mapped = factor * (product(current, vector) - product(reflectors, against_updates) - product(updates, against_reflectors))
            update = mapped - 0.5 * factor * jnp.sum(mapped * vector) * vector
            reflectors = reflectors.at[:, inner_index].set(vector)
            updates = updates.at[:, inner_index].set(update)
        current = current - product(reflectors, updates.T) - product(updates, reflectors.T)
    return current
```

```python
import functools
import math

import jax
import jax.numpy as jnp
from jax import lax
from jax.sharding import PartitionSpec as P
import jax.experimental.pallas as pl
import jax.experimental.pallas.tpu as pltpu

REFL = 4
PANELS = 2
STEPS = REFL * PANELS
LANES = 128
BLOCK = 256
SLOTS = 3
PIECES = 8
VMEM = pl.BlockSpec(memory_space=pltpu.VMEM)


def params(mib, **kw):
    return pltpu.CompilerParams(vmem_limit_bytes=mib << 20, **kw)


def total(x):
    return jnp.sum(jnp.sum(x, axis=0, keepdims=True), axis=1, keepdims=True)


def reflector(column, c):
    shape = column.shape
    row = lax.broadcasted_iota(jnp.int32, shape, 0)
    lane = lax.broadcasted_iota(jnp.int32, shape, 1)
    beneath = jnp.where((row > 0) | (lane > c), column, 0.0)
    length = jnp.sqrt(total(beneath * beneath))
    leading = column[0:1, c + 1 : c + 2]
    signed = jnp.where(leading >= 0.0, length, -length)
    vector = beneath + jnp.where((row == 0) & (lane == c + 1), signed, 0.0)
    return vector, 1.0 / (length * (length + jnp.abs(leading)))


def finish(y, vs, ws, factor):
    v = vs[-1]
    inner = total(y * v)
    rest = y
    for vj, wj in zip(vs[:-1], ws):
        on_w = total(wj * v)
        on_v = total(vj * v)
        rest = rest - vj * on_w - wj * on_v
        inner = inner - 2.0 * on_w * on_v
    return factor * rest - (0.5 * factor * factor * inner) * v


def whole_product(recv_ref, y_ref, row_size, col_size):
    half = recv_ref.shape[1]
    for c in range(col_size):
        for h in range(2):
            parts = [recv_ref[r * col_size + c] for r in range(h, row_size, 2)]
            s = parts[0]
            for p in parts[1:]:
                s = s + p
            y_ref[(c * 2 + h) * half : (c * 2 + h + 1) * half, :] = s


def partial_product(pieces, v_ref, c_ref, p_ref, keep_ref, send_ref, arrive=None):
    height, cols = pieces[0].shape
    tiles = cols // LANES
    lines = height * len(pieces) // LANES
    start = pl.multiple_of(lax.axis_index("row") * lines, 8)
    own = v_ref[pl.ds(start, lines), :]
    turned = jnp.concatenate([own] * (LANES // lines), axis=0).T
    for k in range(lines):
        c_ref[k * LANES : (k + 1) * LANES, :] = jnp.broadcast_to(turned[:, k : k + 1], (LANES, LANES))
    acc = (jnp.zeros((8, LANES), jnp.float32),) * tiles
    for index, a_ref in enumerate(pieces):
        if arrive is not None:
            arrive(index)

        def step(s, acc):
            base = pl.multiple_of(s * LANES, LANES)
            for k in range(0, LANES, 8):
                coef = c_ref[pl.ds(index * height + base + k, 8), :]
                acc = tuple(
                    acc[j] + a_ref[pl.ds(base + k, 8), j * LANES : (j + 1) * LANES] * coef
                    for j in range(tiles)
                )
            return acc

        acc = lax.fori_loop(0, height // LANES, step, acc)
    for j in range(tiles):
        p_ref[j : j + 1, :] = jnp.sum(acc[j], axis=0, keepdims=True)
    half = tiles // 2
    first = lax.axis_index("row") % 2 == 0
    low = p_ref[0:half, :]
    high = p_ref[half:tiles, :]
    keep_ref[...] = jnp.where(first, low, high)
    send_ref[...] = jnp.where(first, high, low)


def first_kernel(a_ref, recv_ref, *refs, count, col_size, shares):
    pieces = refs[:count]
    b_ref, v_ref, f_ref, keep_ref, send_ref, c_ref, p_ref, sems = refs[count:]
    height = pieces[0].shape[0]
    copies = [
        pltpu.make_async_copy(a_ref.at[k * height : (k + 1) * height], pieces[k], sems.at[k])
        for k in range(count)
    ]
    for copy in copies:
        copy.start()
    width = recv_ref.shape[2] // LANES
    for r in range(shares):
        for c in range(col_size):
            for q in range(width):
                b_ref[:, (c * shares + r) * width + q, :] = recv_ref[
                    r * col_size + c, :, q * LANES : (q + 1) * LANES
                ]
    v, factor = reflector(b_ref[0], 0)
    v_ref[...] = v
    f_ref[...] = jnp.broadcast_to(factor, f_ref.shape)
    partial_product(
        pieces, v_ref, c_ref, p_ref, keep_ref, send_ref, lambda k: copies[k].wait()
    )


def next_kernel(*refs, c, count, row_size, col_size):
    pieces = refs[:count]
    recv_ref, b_ref, of_ref = refs[count : count + 3]
    refs = refs[count + 3 :]
    vs = refs[:c]
    ws = refs[c : 2 * c - 1]
    w_ref, v_ref, f_ref, keep_ref, send_ref, y_ref, c_ref, p_ref = refs[2 * c - 1 :]
    whole_product(recv_ref, y_ref, row_size, col_size)
    vs = [r[...] for r in vs]
    ws = [r[...] for r in ws]
    w = finish(y_ref[...], vs, ws, of_ref[0:1, 0:1])
    w_ref[...] = w
    ws = ws + [w]
    column = b_ref[c]
    for vj, wj in zip(vs, ws):
        column = column - vj * wj[0:1, c : c + 1] - wj * vj[0:1, c : c + 1]
    v, factor = reflector(column, c)
    v_ref[...] = v
    f_ref[...] = jnp.broadcast_to(factor, f_ref.shape)
    partial_product(pieces, v_ref, c_ref, p_ref, keep_ref, send_ref)


def spread_kernel(keep_ref, got_ref, out_ref):
    out_ref[...] = jnp.broadcast_to((keep_ref[...] + got_ref[...])[None], out_ref.shape)


def thirds(x):
    hi = x.astype(jnp.bfloat16)
    rest = x - hi.astype(jnp.float32)
    mid = rest.astype(jnp.bfloat16)
    low = (rest - mid.astype(jnp.float32)).astype(jnp.bfloat16)
    return hi, mid, low


def last_kernel(*refs, count, row_size, col_size):
    pieces = refs[:count]
    recv_ref, of_ref = refs[count : count + 2]
    refs = refs[count + 2 :]
    vs = refs[:STEPS]
    ws = refs[STEPS : 2 * STEPS - 1]
    out_ref, y_ref, v_ref, w_ref, left_ref, right_ref, stage_ref, sems = refs[2 * STEPS - 1 :]
    height, cols = pieces[0].shape
    rows = height * count
    slots, block = stage_ref.shape[:2]
    whole_product(recv_ref, y_ref, row_size, col_size)
    v_all = [r[...] for r in vs]
    w_all = [r[...] for r in ws]
    w_all.append(finish(y_ref[...], v_all, w_all, of_ref[0:1, 0:1]))
    for j in range(STEPS):
        v_ref[j] = v_all[j]
        w_ref[j] = w_all[j]
    row_start = lax.axis_index("row") * (rows // LANES)
    for t in range(rows // LANES):
        v = v_ref[:, row_start + t, :]
        w = w_ref[:, row_start + t, :]
        hi, mid, low = thirds(jnp.concatenate([v, w], axis=0))
        left_ref[:, t * LANES : (t + 1) * LANES] = jnp.concatenate([hi, hi, mid, hi, mid, low], axis=0)
    col_start = lax.axis_index("col") * (cols // LANES)
    for t in range(cols // LANES):
        v = v_ref[:, col_start + t, :]
        w = w_ref[:, col_start + t, :]
        hi, mid, low = thirds(jnp.concatenate([w, v], axis=0))
        right_ref[:, t * LANES : (t + 1) * LANES] = jnp.concatenate([hi, mid, hi, low, mid, hi], axis=0)

    def copy(n):
        slot = n % slots
        return pltpu.make_async_copy(
            stage_ref.at[slot], out_ref.at[n * block : (n + 1) * block], sems.at[slot]
        )

    for n in range(rows // block):
        if n >= slots:
            copy(n - slots).wait()
        change = lax.dot_general(
            left_ref[:, n * block : (n + 1) * block],
            right_ref[...],
            (((0,), (0,)), ((), ())),
            preferred_element_type=jnp.float32,
        )
        at = n * block
        stage_ref[n % slots] = pieces[at // height][at % height : at % height + block, :] - change
        copy(n).start()
    for n in range(max(0, rows // block - slots), rows // block):
        copy(n).wait()


def f32(*shape):
    return jax.ShapeDtypeStruct(shape, jnp.float32)


def on_device(matrix):
    rows, cols = matrix.shape
    row_size = lax.axis_size("row")
    col_size = lax.axis_size("col")
    lines = rows * row_size // LANES
    tiles = cols // LANES
    both = ("row", "col")
    everyone = row_size * col_size
    pairs = [(i, i ^ 1) for i in range(row_size)]
    scratch = [pltpu.VMEM((rows, LANES), jnp.float32), pltpu.VMEM((tiles, LANES), jnp.float32)]
    state = [f32(lines, LANES), f32(8, LANES), f32(tiles // 2, LANES), f32(tiles // 2, LANES)]

    shares = math.gcd(row_size, tiles)
    width = cols // shares
    head = matrix[:STEPS, :].reshape(STEPS, shares, width).transpose(1, 0, 2)
    head = jnp.concatenate([head] * (row_size // shares), axis=0)
    mine = lax.all_to_all(head, "row", 0, 0, tiled=True)[0]
    heads = lax.all_to_all(
        jnp.broadcast_to(mine[None], (everyone,) + mine.shape), both, 0, 0, tiled=True
    )
    count = math.gcd(PIECES, rows // LANES)
    pieces = [pltpu.VMEM((rows // count, cols), jnp.float32)] * count

    def exchange(keep, send):
        got = lax.ppermute(send, "row", pairs)
        spread = pl.pallas_call(
            spread_kernel,
            out_shape=f32(everyone, *keep.shape),
            in_specs=[VMEM] * 2,
            out_specs=VMEM,
            compiler_params=params(4),
            name="spread",
        )(keep, got)
        return lax.all_to_all(spread, both, 0, 0, tiled=True)

    *held, top, v, factor, keep, send = pl.pallas_call(
        functools.partial(first_kernel, count=count, col_size=col_size, shares=shares),
        out_shape=pieces + [f32(STEPS, lines, LANES)] + state,
        in_specs=[pl.BlockSpec(memory_space=pl.ANY), VMEM],
        out_specs=[VMEM] * (count + 5),
        scratch_shapes=scratch + [pltpu.SemaphoreType.DMA((count,))],
        compiler_params=params(6),
        name="first",
    )(matrix, heads)
    vs, ws = [v], []
    for c in range(1, STEPS):
        recv = exchange(keep, send)
        w, v, factor, keep, send = pl.pallas_call(
            functools.partial(
                next_kernel, c=c, count=count, row_size=row_size, col_size=col_size
            ),
            out_shape=[f32(lines, LANES)] + state,
            in_specs=[VMEM] * (count + 2 + 2 * c),
            out_specs=[VMEM] * 5,
            scratch_shapes=[pltpu.VMEM((lines, LANES), jnp.float32)] + scratch,
            compiler_params=params(6),
            name=f"next{c}",
        )(*held, recv, top, factor, *vs, *ws)
        ws.append(w)
        vs.append(v)
    recv = exchange(keep, send)
    block = math.gcd(rows // count, BLOCK)
    return pl.pallas_call(
        functools.partial(last_kernel, count=count, row_size=row_size, col_size=col_size),
        out_shape=f32(rows, cols),
        in_specs=[VMEM] * (count + 1 + 2 * STEPS),
        out_specs=pl.BlockSpec(memory_space=pl.ANY),
        scratch_shapes=[
            pltpu.VMEM((lines, LANES), jnp.float32),
            pltpu.VMEM((STEPS, lines, LANES), jnp.float32),
            pltpu.VMEM((STEPS, lines, LANES), jnp.float32),
            pltpu.VMEM((12 * STEPS, rows), jnp.bfloat16),
            pltpu.VMEM((12 * STEPS, cols), jnp.bfloat16),
            pltpu.VMEM((SLOTS, block, cols), jnp.float32),
            pltpu.SemaphoreType.DMA((SLOTS,)),
        ],
        compiler_params=params(10),
        name="last",
    )(*held, recv, factor, *vs, *ws)


def solution(mesh):
    return jax.shard_map(
        on_device,
        mesh=mesh,
        in_specs=(P("row", "col"),),
        out_specs=P("row", "col"),
        check_vma=False,
    )
```

```python
import functools
import math

import jax
import jax.numpy as jnp
from jax import lax
from jax.sharding import PartitionSpec as P
import jax.experimental.pallas as pl
import jax.experimental.pallas.tpu as pltpu

REFL = 4
PANELS = 2
STEPS = REFL * PANELS
LANES = 128
BLOCK = 256
SLOTS = 3
PIECES = 8
EARLY = 2
MIDDLE = 4
VMEM = pl.BlockSpec(memory_space=pltpu.VMEM)
HBM = pl.BlockSpec(memory_space=pltpu.HBM)


def params(mib, **kw):
    return pltpu.CompilerParams(vmem_limit_bytes=mib << 20, **kw)


def total(x):
    return jnp.sum(jnp.sum(x, axis=0, keepdims=True), axis=1, keepdims=True)


def reflector(column, c):
    shape = column.shape
    row = lax.broadcasted_iota(jnp.int32, shape, 0)
    lane = lax.broadcasted_iota(jnp.int32, shape, 1)
    beneath = jnp.where((row > 0) | (lane > c), column, 0.0)
    length = jnp.sqrt(total(beneath * beneath))
    leading = column[0:1, c + 1 : c + 2]
    signed = jnp.where(leading >= 0.0, length, -length)
    vector = beneath + jnp.where((row == 0) & (lane == c + 1), signed, 0.0)
    return vector, 1.0 / (length * (length + jnp.abs(leading)))


def finish(y, vs, ws, factor):
    v = vs[-1]
    inner = total(y * v)
    rest = y
    for vj, wj in zip(vs[:-1], ws):
        on_w = total(wj * v)
        on_v = total(vj * v)
        rest = rest - vj * on_w - wj * on_v
        inner = inner - 2.0 * on_w * on_v
    return factor * rest - (0.5 * factor * factor * inner) * v


def whole_product(recv_ref, y_ref, row_size, col_size):
    half = recv_ref.shape[1]
    for c in range(col_size):
        for h in range(2):
            parts = [recv_ref[r * col_size + c] for r in range(h, row_size, 2)]
            s = parts[0]
            for p in parts[1:]:
                s = s + p
            y_ref[(c * 2 + h) * half : (c * 2 + h + 1) * half, :] = s


def partial_product(pieces, v_ref, c_ref, p_ref, keep_ref, send_ref, arrive=None):
    height, cols = pieces[0].shape
    tiles = cols // LANES
    lines = height * len(pieces) // LANES
    start = pl.multiple_of(lax.axis_index("row") * lines, 8)
    own = v_ref[pl.ds(start, lines), :]
    turned = jnp.concatenate([own] * (LANES // lines), axis=0).T
    for k in range(lines):
        c_ref[k * LANES : (k + 1) * LANES, :] = jnp.broadcast_to(turned[:, k : k + 1], (LANES, LANES))
    acc = (jnp.zeros((8, LANES), jnp.float32),) * tiles
    for index, a_ref in enumerate(pieces):
        if arrive is not None:
            arrive(index)

        def step(s, acc):
            base = pl.multiple_of(s * LANES, LANES)
            for k in range(0, LANES, 8):
                coef = c_ref[pl.ds(index * height + base + k, 8), :]
                acc = tuple(
                    acc[j] + a_ref[pl.ds(base + k, 8), j * LANES : (j + 1) * LANES] * coef
                    for j in range(tiles)
                )
            return acc

        acc = lax.fori_loop(0, height // LANES, step, acc)
    for j in range(tiles):
        p_ref[j : j + 1, :] = jnp.sum(acc[j], axis=0, keepdims=True)
    half = tiles // 2
    first = lax.axis_index("row") % 2 == 0
    low = p_ref[0:half, :]
    high = p_ref[half:tiles, :]
    keep_ref[...] = jnp.where(first, low, high)
    send_ref[...] = jnp.where(first, high, low)


def piece_copies(a_ref, pieces, sems, start):
    height = pieces[0].shape[0]
    return [
        pltpu.make_async_copy(
            a_ref.at[(start + k) * height : (start + k + 1) * height], piece, sems.at[k]
        )
        for k, piece in enumerate(pieces)
    ]


def load_kernel(a_ref, *refs, skip, start):
    copies = piece_copies(a_ref, refs[skip:-1], refs[-1], start)
    for copy in copies:
        copy.start()
    for copy in copies:
        copy.wait()


def head_kernel(*refs):
    own_ref, out_ref = refs[1], refs[-1]
    mine = jnp.where(lax.axis_index("row") == 0, own_ref[...], 0.0)
    for got_ref in refs[2:-1]:
        mine = mine + got_ref[...]
    out_ref[...] = jnp.broadcast_to(mine[None], out_ref.shape)


def first_kernel(a_ref, *refs, early, count, col_size, shares):
    pieces = refs[:early]
    near_ref, far_ref = refs[early : early + 2]
    late = refs[early + 2 : count + 2]
    b_ref, v_ref, f_ref, keep_ref, send_ref, c_ref, p_ref, sems = refs[count + 2 :]
    copies = piece_copies(a_ref, late, sems, early)
    for copy in copies:
        copy.start()
    pieces = pieces + late
    width = near_ref.shape[2] // LANES
    even = lax.axis_index("row") % 2 == 0
    for r in range(shares):
        for c in range(col_size):
            near = near_ref[(r // 2) * col_size + c]
            far = far_ref[(r // 2) * col_size + c]
            piece = jnp.where(even, near, far) if r % 2 == 0 else jnp.where(even, far, near)
            for q in range(width):
                b_ref[:, (c * shares + r) * width + q, :] = piece[:, q * LANES : (q + 1) * LANES]
    v, factor = reflector(b_ref[0], 0)
    v_ref[...] = v
    f_ref[...] = jnp.broadcast_to(factor, f_ref.shape)
    partial_product(
        pieces,
        v_ref,
        c_ref,
        p_ref,
        keep_ref,
        send_ref,
        lambda k: copies[k - early].wait() if k >= early else None,
    )


def next_kernel(*refs, c, count, row_size, col_size):
    pieces = refs[:count]
    recv_ref, b_ref, of_ref = refs[count : count + 3]
    refs = refs[count + 3 :]
    vs = refs[:c]
    ws = refs[c : 2 * c - 1]
    w_ref, v_ref, f_ref, keep_ref, send_ref, y_ref, c_ref, p_ref = refs[2 * c - 1 :]
    whole_product(recv_ref, y_ref, row_size, col_size)
    vs = [r[...] for r in vs]
    ws = [r[...] for r in ws]
    w = finish(y_ref[...], vs, ws, of_ref[0:1, 0:1])
    w_ref[...] = w
    ws = ws + [w]
    column = b_ref[c]
    for vj, wj in zip(vs, ws):
        column = column - vj * wj[0:1, c : c + 1] - wj * vj[0:1, c : c + 1]
    v, factor = reflector(column, c)
    v_ref[...] = v
    f_ref[...] = jnp.broadcast_to(factor, f_ref.shape)
    partial_product(pieces, v_ref, c_ref, p_ref, keep_ref, send_ref)


def spread_kernel(keep_ref, got_ref, out_ref):
    out_ref[...] = jnp.broadcast_to((keep_ref[...] + got_ref[...])[None], out_ref.shape)


def thirds(x):
    hi = x.astype(jnp.bfloat16)
    rest = x - hi.astype(jnp.float32)
    mid = rest.astype(jnp.bfloat16)
    low = (rest - mid.astype(jnp.float32)).astype(jnp.bfloat16)
    return hi, mid, low


def last_kernel(*refs, count, row_size, col_size):
    pieces = refs[:count]
    recv_ref, of_ref = refs[count : count + 2]
    refs = refs[count + 2 :]
    vs = refs[:STEPS]
    ws = refs[STEPS : 2 * STEPS - 1]
    out_ref, y_ref, v_ref, w_ref, left_ref, right_ref, stage_ref, sems = refs[2 * STEPS - 1 :]
    height, cols = pieces[0].shape
    rows = height * count
    slots, block = stage_ref.shape[:2]
    whole_product(recv_ref, y_ref, row_size, col_size)
    v_all = [r[...] for r in vs]
    w_all = [r[...] for r in ws]
    w_all.append(finish(y_ref[...], v_all, w_all, of_ref[0:1, 0:1]))
    for j in range(STEPS):
        v_ref[j] = v_all[j]
        w_ref[j] = w_all[j]
    row_start = lax.axis_index("row") * (rows // LANES)
    for t in range(rows // LANES):
        v = v_ref[:, row_start + t, :]
        w = w_ref[:, row_start + t, :]
        hi, mid, low = thirds(jnp.concatenate([v, w], axis=0))
        left_ref[:, t * LANES : (t + 1) * LANES] = jnp.concatenate([hi, hi, mid, hi, mid, low], axis=0)
    col_start = lax.axis_index("col") * (cols // LANES)
    for t in range(cols // LANES):
        v = v_ref[:, col_start + t, :]
        w = w_ref[:, col_start + t, :]
        hi, mid, low = thirds(jnp.concatenate([w, v], axis=0))
        right_ref[:, t * LANES : (t + 1) * LANES] = jnp.concatenate([hi, mid, hi, low, mid, hi], axis=0)

    def copy(n):
        slot = n % slots
        return pltpu.make_async_copy(
            stage_ref.at[slot], out_ref.at[n * block : (n + 1) * block], sems.at[slot]
        )

    for n in range(rows // block):
        if n >= slots:
            copy(n - slots).wait()
        change = lax.dot_general(
            left_ref[:, n * block : (n + 1) * block],
            right_ref[...],
            (((0,), (0,)), ((), ())),
            preferred_element_type=jnp.float32,
        )
        at = n * block
        stage_ref[n % slots] = pieces[at // height][at % height : at % height + block, :] - change
        copy(n).start()
    for n in range(max(0, rows // block - slots), rows // block):
        copy(n).wait()


def f32(*shape):
    return jax.ShapeDtypeStruct(shape, jnp.float32)


def on_device(matrix):
    rows, cols = matrix.shape
    row_size = lax.axis_size("row")
    col_size = lax.axis_size("col")
    lines = rows * row_size // LANES
    tiles = cols // LANES
    both = ("row", "col")
    everyone = row_size * col_size
    pairs = [(i, i ^ 1) for i in range(row_size)]
    scratch = [pltpu.VMEM((rows, LANES), jnp.float32), pltpu.VMEM((tiles, LANES), jnp.float32)]
    state = [f32(lines, LANES), f32(8, LANES), f32(tiles // 2, LANES), f32(tiles // 2, LANES)]

    count = math.gcd(PIECES, rows // LANES)
    pieces = [pltpu.VMEM((rows // count, cols), jnp.float32)] * count

    shares = math.gcd(row_size, tiles)
    width = cols // shares
    own = matrix[:STEPS, :width]
    gots = []
    for r in range(1, shares):
        part = matrix[:STEPS, r * width : (r + 1) * width]
        gots.append(lax.ppermute(part, "row", [(0, r)]))
    early = min(EARLY, count - 1)
    middle = min(MIDDLE, count - 1)

    def load(start, stop, *after):
        return pl.pallas_call(
            functools.partial(load_kernel, skip=len(after), start=start),
            out_shape=pieces[start:stop],
            in_specs=[HBM] + [VMEM] * len(after),
            out_specs=[VMEM] * (stop - start),
            scratch_shapes=[pltpu.SemaphoreType.DMA((stop - start,))],
            compiler_params=params(24),
            cost_estimate=pl.CostEstimate(
                flops=(stop - start) << 28, bytes_accessed=0, transcendentals=0
            ),
            name=f"load{start}",
        )(matrix, *after)

    loaded = load(0, early)
    same = everyone // 2
    heads = pl.pallas_call(
        head_kernel,
        out_shape=f32(same, STEPS, width),
        in_specs=[VMEM] * (shares + 1),
        out_specs=VMEM,
        compiler_params=params(4),
        name="head",
    )(loaded[0], own, *gots)
    groups = [
        [r * col_size + c for r in range(core, row_size, 2) for c in range(col_size)]
        for core in range(2)
    ]
    near = lax.all_to_all(heads, both, 0, 0, tiled=True, axis_index_groups=groups)
    far = lax.ppermute(near, "row", pairs)
    if middle > early:
        loaded = [*loaded, *load(early, middle, near)]

    def exchange(keep, send):
        got = lax.ppermute(send, "row", pairs)
        spread = pl.pallas_call(
            spread_kernel,
            out_shape=f32(everyone, *keep.shape),
            in_specs=[VMEM] * 2,
            out_specs=VMEM,
            compiler_params=params(4),
            name="spread",
        )(keep, got)
        return lax.all_to_all(spread, both, 0, 0, tiled=True)

    *held, top, v, factor, keep, send = pl.pallas_call(
        functools.partial(
            first_kernel, early=middle, count=count, col_size=col_size, shares=shares
        ),
        out_shape=pieces[middle:] + [f32(STEPS, lines, LANES)] + state,
        in_specs=[HBM] + [VMEM] * (middle + 2),
        out_specs=[VMEM] * (count - middle + 5),
        scratch_shapes=scratch + [pltpu.SemaphoreType.DMA((count - middle,))],
        compiler_params=params(6),
        name="first",
    )(matrix, *loaded, near, far)
    held = [*loaded, *held]
    vs, ws = [v], []
    for c in range(1, STEPS):
        recv = exchange(keep, send)
        w, v, factor, keep, send = pl.pallas_call(
            functools.partial(
                next_kernel, c=c, count=count, row_size=row_size, col_size=col_size
            ),
            out_shape=[f32(lines, LANES)] + state,
            in_specs=[VMEM] * (count + 2 + 2 * c),
            out_specs=[VMEM] * 5,
            scratch_shapes=[pltpu.VMEM((lines, LANES), jnp.float32)] + scratch,
            compiler_params=params(6),
            name=f"next{c}",
        )(*held, recv, top, factor, *vs, *ws)
        ws.append(w)
        vs.append(v)
    recv = exchange(keep, send)
    block = math.gcd(rows // count, BLOCK)
    return pl.pallas_call(
        functools.partial(last_kernel, count=count, row_size=row_size, col_size=col_size),
        out_shape=f32(rows, cols),
        in_specs=[VMEM] * (count + 1 + 2 * STEPS),
        out_specs=HBM,
        scratch_shapes=[
            pltpu.VMEM((lines, LANES), jnp.float32),
            pltpu.VMEM((STEPS, lines, LANES), jnp.float32),
            pltpu.VMEM((STEPS, lines, LANES), jnp.float32),
            pltpu.VMEM((12 * STEPS, rows), jnp.bfloat16),
            pltpu.VMEM((12 * STEPS, cols), jnp.bfloat16),
            pltpu.VMEM((SLOTS, block, cols), jnp.float32),
            pltpu.SemaphoreType.DMA((SLOTS,)),
        ],
        compiler_params=params(10),
        name="last",
    )(*held, recv, factor, *vs, *ws)


def solution(mesh):
    return jax.shard_map(
        on_device,
        mesh=mesh,
        in_specs=(P("row", "col"),),
        out_specs=P("row", "col"),
        check_vma=False,
    )
```

```python
import functools
import math

import jax
import jax.numpy as jnp
from jax import lax
from jax.sharding import PartitionSpec as P
import jax.experimental.pallas as pl
import jax.experimental.pallas.tpu as pltpu

REFL = 4
PANELS = 2
STEPS = REFL * PANELS
LANES = 128
BLOCK = 256
SLOTS = 3
PIECES = 8
EARLY = 2
MIDDLE = 4
VMEM = pl.BlockSpec(memory_space=pltpu.VMEM)
HBM = pl.BlockSpec(memory_space=pltpu.HBM)


def params(mib, **kw):
    return pltpu.CompilerParams(vmem_limit_bytes=mib << 20, **kw)


def total(x):
    return jnp.sum(jnp.sum(x, axis=0, keepdims=True), axis=1, keepdims=True)


def reflector(column, c):
    shape = column.shape
    row = lax.broadcasted_iota(jnp.int32, shape, 0)
    lane = lax.broadcasted_iota(jnp.int32, shape, 1)
    beneath = jnp.where((row > 0) | (lane > c), column, 0.0)
    length = jnp.sqrt(total(beneath * beneath))
    leading = column[0:1, c + 1 : c + 2]
    signed = jnp.where(leading >= 0.0, length, -length)
    vector = beneath + jnp.where((row == 0) & (lane == c + 1), signed, 0.0)
    return vector, 1.0 / (length * (length + jnp.abs(leading)))


def finish(y, vs, ws, factor):
    v = vs[-1]
    inner = total(y * v)
    rest = y
    for vj, wj in zip(vs[:-1], ws):
        on_w = total(wj * v)
        on_v = total(vj * v)
        rest = rest - vj * on_w - wj * on_v
        inner = inner - 2.0 * on_w * on_v
    return factor * rest - (0.5 * factor * factor * inner) * v


def whole_product(recv_ref, y_ref, row_size, col_size):
    half = recv_ref.shape[1]
    sums = []
    for c in range(col_size):
        for h in range(2):
            parts = [recv_ref[r * col_size + c] for r in range(h, row_size, 2)]
            s = parts[0]
            for p in parts[1:]:
                s = s + p
            sums.append(s)
    if half % 8 == 0:
        return jnp.concatenate(sums, axis=0)
    for k, s in enumerate(sums):
        y_ref[k * half : (k + 1) * half, :] = s
    return y_ref[...]


def partial_product(pieces, v_ref, c_ref, p_ref, keep_ref, send_ref, arrive=None):
    height, cols = pieces[0].shape
    tiles = cols // LANES
    lines = height * len(pieces) // LANES
    start = pl.multiple_of(lax.axis_index("row") * lines, 8)
    own = v_ref[pl.ds(start, lines), :]
    turned = jnp.concatenate([own] * (LANES // lines), axis=0).T
    for k in range(lines):
        c_ref[k * LANES : (k + 1) * LANES, :] = jnp.broadcast_to(turned[:, k : k + 1], (LANES, LANES))
    acc = (jnp.zeros((8, LANES), jnp.float32),) * tiles
    for index, a_ref in enumerate(pieces):
        if arrive is not None:
            arrive(index)

        def step(s, acc):
            base = pl.multiple_of(s * LANES, LANES)
            for k in range(0, LANES, 8):
                coef = c_ref[pl.ds(index * height + base + k, 8), :]
                acc = tuple(
                    acc[j] + a_ref[pl.ds(base + k, 8), j * LANES : (j + 1) * LANES] * coef
                    for j in range(tiles)
                )
            return acc

        acc = lax.fori_loop(0, height // LANES, step, acc)
    for j in range(tiles):
        p_ref[j : j + 1, :] = jnp.sum(acc[j], axis=0, keepdims=True)
    half = tiles // 2
    first = lax.axis_index("row") % 2 == 0
    low = p_ref[0:half, :]
    high = p_ref[half:tiles, :]
    keep_ref[...] = jnp.where(first, low, high)
    send_ref[...] = jnp.where(first, high, low)


def piece_copies(a_ref, pieces, sems, start):
    height = pieces[0].shape[0]
    return [
        pltpu.make_async_copy(
            a_ref.at[(start + k) * height : (start + k + 1) * height], piece, sems.at[k]
        )
        for k, piece in enumerate(pieces)
    ]


def load_kernel(a_ref, *refs, skip, start):
    copies = piece_copies(a_ref, refs[skip:-1], refs[-1], start)
    for copy in copies:
        copy.start()
    for copy in copies:
        copy.wait()


def head_kernel(*refs):
    own_ref, out_ref = refs[1], refs[-1]
    mine = jnp.where(lax.axis_index("row") == 0, own_ref[...], 0.0)
    for got_ref in refs[2:-1]:
        mine = mine + got_ref[...]
    out_ref[...] = jnp.broadcast_to(mine[None], out_ref.shape)


def first_kernel(a_ref, *refs, early, count, col_size, shares):
    pieces = refs[:early]
    near_ref, far_ref = refs[early : early + 2]
    late = refs[early + 2 : count + 2]
    b_ref, v_ref, f_ref, keep_ref, send_ref, c_ref, p_ref, sems = refs[count + 2 :]
    copies = piece_copies(a_ref, late, sems, early)
    for copy in copies:
        copy.start()
    pieces = pieces + late
    width = near_ref.shape[2] // LANES
    even = lax.axis_index("row") % 2 == 0
    for r in range(shares):
        for c in range(col_size):
            near = near_ref[(r // 2) * col_size + c]
            far = far_ref[(r // 2) * col_size + c]
            piece = jnp.where(even, near, far) if r % 2 == 0 else jnp.where(even, far, near)
            for q in range(width):
                b_ref[:, (c * shares + r) * width + q, :] = piece[:, q * LANES : (q + 1) * LANES]
    v, factor = reflector(b_ref[0], 0)
    v_ref[...] = v
    f_ref[...] = jnp.broadcast_to(factor, f_ref.shape)
    partial_product(
        pieces,
        v_ref,
        c_ref,
        p_ref,
        keep_ref,
        send_ref,
        lambda k: copies[k - early].wait() if k >= early else None,
    )


def next_kernel(*refs, c, count, row_size, col_size):
    pieces = refs[:count]
    recv_ref, b_ref, of_ref = refs[count : count + 3]
    refs = refs[count + 3 :]
    vs = refs[:c]
    ws = refs[c : 2 * c - 1]
    w_ref, v_ref, f_ref, keep_ref, send_ref, y_ref, c_ref, p_ref = refs[2 * c - 1 :]
    y = whole_product(recv_ref, y_ref, row_size, col_size)
    vs = [r[...] for r in vs]
    ws = [r[...] for r in ws]
    w = finish(y, vs, ws, of_ref[0:1, 0:1])
    w_ref[...] = w
    ws = ws + [w]
    column = b_ref[c]
    for vj, wj in zip(vs, ws):
        column = column - vj * wj[0:1, c : c + 1] - wj * vj[0:1, c : c + 1]
    v, factor = reflector(column, c)
    v_ref[...] = v
    f_ref[...] = jnp.broadcast_to(factor, f_ref.shape)
    partial_product(pieces, v_ref, c_ref, p_ref, keep_ref, send_ref)


def spread_kernel(keep_ref, got_ref, out_ref):
    out_ref[...] = jnp.broadcast_to((keep_ref[...] + got_ref[...])[None], out_ref.shape)


def thirds(x):
    hi = x.astype(jnp.bfloat16)
    rest = x - hi.astype(jnp.float32)
    mid = rest.astype(jnp.bfloat16)
    low = (rest - mid.astype(jnp.float32)).astype(jnp.bfloat16)
    return hi, mid, low


def last_kernel(*refs, count, row_size, col_size):
    pieces = refs[:count]
    recv_ref, of_ref = refs[count : count + 2]
    refs = refs[count + 2 :]
    vs = refs[:STEPS]
    ws = refs[STEPS : 2 * STEPS - 1]
    out_ref, y_ref, v_ref, w_ref, left_ref, right_ref, stage_ref, sems = refs[2 * STEPS - 1 :]
    height, cols = pieces[0].shape
    rows = height * count
    slots, block = stage_ref.shape[:2]
    y = whole_product(recv_ref, y_ref, row_size, col_size)
    v_all = [r[...] for r in vs]
    w_all = [r[...] for r in ws]
    w_all.append(finish(y, v_all, w_all, of_ref[0:1, 0:1]))
    for j in range(STEPS):
        v_ref[j] = v_all[j]
        w_ref[j] = w_all[j]
    row_start = lax.axis_index("row") * (rows // LANES)
    for t in range(rows // LANES):
        v = v_ref[:, row_start + t, :]
        w = w_ref[:, row_start + t, :]
        hi, mid, low = thirds(jnp.concatenate([v, w], axis=0))
        left_ref[:, t * LANES : (t + 1) * LANES] = jnp.concatenate([hi, hi, mid, hi, mid, low], axis=0)
    col_start = lax.axis_index("col") * (cols // LANES)
    for t in range(cols // LANES):
        v = v_ref[:, col_start + t, :]
        w = w_ref[:, col_start + t, :]
        hi, mid, low = thirds(jnp.concatenate([w, v], axis=0))
        right_ref[:, t * LANES : (t + 1) * LANES] = jnp.concatenate([hi, mid, hi, low, mid, hi], axis=0)

    def copy(n):
        slot = n % slots
        return pltpu.make_async_copy(
            stage_ref.at[slot], out_ref.at[n * block : (n + 1) * block], sems.at[slot]
        )

    for n in range(rows // block):
        if n >= slots:
            copy(n - slots).wait()
        change = lax.dot_general(
            left_ref[:, n * block : (n + 1) * block],
            right_ref[...],
            (((0,), (0,)), ((), ())),
            preferred_element_type=jnp.float32,
        )
        at = n * block
        stage_ref[n % slots] = pieces[at // height][at % height : at % height + block, :] - change
        copy(n).start()
    for n in range(max(0, rows // block - slots), rows // block):
        copy(n).wait()


def f32(*shape):
    return jax.ShapeDtypeStruct(shape, jnp.float32)


def on_device(matrix):
    rows, cols = matrix.shape
    row_size = lax.axis_size("row")
    col_size = lax.axis_size("col")
    lines = rows * row_size // LANES
    tiles = cols // LANES
    both = ("row", "col")
    everyone = row_size * col_size
    pairs = [(i, i ^ 1) for i in range(row_size)]
    scratch = [pltpu.VMEM((rows, LANES), jnp.float32), pltpu.VMEM((tiles, LANES), jnp.float32)]
    state = [f32(lines, LANES), f32(8, LANES), f32(tiles // 2, LANES), f32(tiles // 2, LANES)]

    count = math.gcd(PIECES, rows // LANES)
    pieces = [pltpu.VMEM((rows // count, cols), jnp.float32)] * count

    shares = math.gcd(row_size, tiles)
    width = cols // shares
    own = matrix[:STEPS, :width]
    gots = []
    for r in range(1, shares):
        part = matrix[:STEPS, r * width : (r + 1) * width]
        gots.append(lax.ppermute(part, "row", [(0, r)]))
    early = min(EARLY, count - 1)
    middle = min(MIDDLE, count - 1)

    def load(start, stop, *after):
        return pl.pallas_call(
            functools.partial(load_kernel, skip=len(after), start=start),
            out_shape=pieces[start:stop],
            in_specs=[HBM] + [VMEM] * len(after),
            out_specs=[VMEM] * (stop - start),
            scratch_shapes=[pltpu.SemaphoreType.DMA((stop - start,))],
            compiler_params=params(24),
            cost_estimate=pl.CostEstimate(
                flops=(stop - start) << 28, bytes_accessed=0, transcendentals=0
            ),
            name=f"load{start}",
        )(matrix, *after)

    loaded = load(0, early)
    same = everyone // 2
    heads = pl.pallas_call(
        head_kernel,
        out_shape=f32(same, STEPS, width),
        in_specs=[VMEM] * (shares + 1),
        out_specs=VMEM,
        compiler_params=params(4),
        name="head",
    )(loaded[0], own, *gots)
    groups = [
        [r * col_size + c for r in range(core, row_size, 2) for c in range(col_size)]
        for core in range(2)
    ]
    near = lax.all_to_all(heads, both, 0, 0, tiled=True, axis_index_groups=groups)
    far = lax.ppermute(near, "row", pairs)
    if middle > early:
        loaded = [*loaded, *load(early, middle, near)]

    def exchange(keep, send):
        got = lax.ppermute(send, "row", pairs)
        spread = pl.pallas_call(
            spread_kernel,
            out_shape=f32(everyone, *keep.shape),
            in_specs=[VMEM] * 2,
            out_specs=VMEM,
            compiler_params=params(4),
            name="spread",
        )(keep, got)
        return lax.all_to_all(spread, both, 0, 0, tiled=True)

    *held, top, v, factor, keep, send = pl.pallas_call(
        functools.partial(
            first_kernel, early=middle, count=count, col_size=col_size, shares=shares
        ),
        out_shape=pieces[middle:] + [f32(STEPS, lines, LANES)] + state,
        in_specs=[HBM] + [VMEM] * (middle + 2),
        out_specs=[VMEM] * (count - middle + 5),
        scratch_shapes=scratch + [pltpu.SemaphoreType.DMA((count - middle,))],
        compiler_params=params(6),
        name="first",
    )(matrix, *loaded, near, far)
    held = [*loaded, *held]
    vs, ws = [v], []
    for c in range(1, STEPS):
        recv = exchange(keep, send)
        w, v, factor, keep, send = pl.pallas_call(
            functools.partial(
                next_kernel, c=c, count=count, row_size=row_size, col_size=col_size
            ),
            out_shape=[f32(lines, LANES)] + state,
            in_specs=[VMEM] * (count + 2 + 2 * c),
            out_specs=[VMEM] * 5,
            scratch_shapes=[pltpu.VMEM((lines, LANES), jnp.float32)] + scratch,
            compiler_params=params(6),
            name=f"next{c}",
        )(*held, recv, top, factor, *vs, *ws)
        ws.append(w)
        vs.append(v)
    recv = exchange(keep, send)
    block = math.gcd(rows // count, BLOCK)
    return pl.pallas_call(
        functools.partial(last_kernel, count=count, row_size=row_size, col_size=col_size),
        out_shape=f32(rows, cols),
        in_specs=[VMEM] * (count + 1 + 2 * STEPS),
        out_specs=HBM,
        scratch_shapes=[
            pltpu.VMEM((lines, LANES), jnp.float32),
            pltpu.VMEM((STEPS, lines, LANES), jnp.float32),
            pltpu.VMEM((STEPS, lines, LANES), jnp.float32),
            pltpu.VMEM((12 * STEPS, rows), jnp.bfloat16),
            pltpu.VMEM((12 * STEPS, cols), jnp.bfloat16),
            pltpu.VMEM((SLOTS, block, cols), jnp.float32),
            pltpu.SemaphoreType.DMA((SLOTS,)),
        ],
        compiler_params=params(10),
        name="last",
    )(*held, recv, factor, *vs, *ws)


def solution(mesh):
    return jax.shard_map(
        on_device,
        mesh=mesh,
        in_specs=(P("row", "col"),),
        out_specs=P("row", "col"),
        check_vma=False,
    )
```
